32 devices in a mesh: grp: 2 (over x), panel: 16 (over z, y, core).
Axes of the slice: x: 2, y: 2, z: 4, core: 2. Of those that a mesh axis runs over, the one named last changes fastest.
Arguments:
- density: bfloat16 [1024, 16, 128], P(('grp', 'panel')), parts along dimension 0, may hold values from -6 to 6
- near_blocks: bfloat16 [1024, 8, 128, 128], P(('grp', 'panel')), parts along dimension 0, may hold values from -0.1875 to 0.1875
- neighbours: int32 [1024, 8], P(('grp', 'panel')), parts along dimension 0, may hold values from 0 to 511, as said below
- counts: int32 [1024], P(('grp', 'panel')), parts along dimension 0, may hold values from 1 to 8, as said below
- coarse_map: int32 [1024], P(('grp', 'panel')), parts along dimension 0, may hold values from 0 to 31, as said below
- restrict: bfloat16 [1024, 128, 128], P(('grp', 'panel')), parts along dimension 0, may hold values from -0.125 to 0.125
- evaluate: bfloat16 [1024, 128, 128], P(('grp', 'panel')), parts along dimension 0, may hold values from -0.5 to 0.5
- coupling: float32 [64, 32], P(('grp', 'panel')), parts along dimension 0, as said below
Outputs:
- potential: bfloat16 [1024, 16, 128], P(('grp', 'panel')), parts along dimension 0
The draws below stay inside these ranges and needn't reach their ends.
There are 2 independent parts, one for each index of `grp`. The reference program is written for one: setup_inputs(seed, part) draws one part's arguments, and reference() takes and returns one part's arrays. A program takes and returns all parts, laid end to end along the dimension named above; each array names one. Nothing has to cross between parts.
Inputs may be any that keep to these rules, and one draw needn't show every extreme that they name: `neighbours`: slot 0 of block b is b itself; every entry lies within 16 blocks of b; in every draw some entry lies exactly 16 blocks below its block and some exactly 16 above. `counts`: every device holds blocks with all 8 slots live. `coarse_map`: block b's coarse cluster is one of the 2 clusters from (b // 32) * 2 on. `coupling`: the matrix is symmetric.
All inputs are finite; a program needn't handle non-finite values.
Results may differ from the reference program's by a relative error of at most 0.0042.
Values may be sent and summed in bfloat16 or wider, within the bound.
No kernel may reach another device: no remote copies, remote signals or barrier semaphores. Data moves between devices by JAX's collectives and lax.ppermute only.
A program may use at most 64 MiB of HBM per device.

```python
import jax
import jax.numpy as jnp
from jax import lax

BLK = 128
RHS = 16
NB = 8
K = 128
COARSE_DEV = 2
BLK_DEV = 32
REACH = 16
NBLK = 512
NCOARSE = 32


def near_tables(key):
    key_offsets = jax.random.fold_in(key, 11)
    key_counts = jax.random.fold_in(key, 12)
    block_rows = jnp.arange(NBLK).astype(jnp.int32)
    offsets = jax.random.randint(key_offsets, (NBLK, NB), -REACH, REACH + 1).astype(jnp.int32)
    within = block_rows % BLK_DEV
    first_row = within == 0
    last_row = within == BLK_DEV - 1
    second = jnp.where(first_row, -REACH, jnp.where(last_row, REACH, offsets[:, 1])).astype(jnp.int32)
    offsets = offsets.at[:, 1].set(second)
    offsets = offsets.at[:, 0].set(0)
    block_ids = jnp.clip(block_rows[:, None] + offsets, 0, NBLK - 1).astype(jnp.int32)
    live_counts = jax.random.randint(key_counts, (NBLK,), 1, NB + 1).astype(jnp.int32)
    live_counts = jnp.where(first_row | last_row, NB, live_counts).astype(jnp.int32)
    return (block_ids, live_counts)


def draw_neighbours(key, part):
    return near_tables(key)[0]


def draw_counts(key, part):
    return near_tables(key)[1]


def draw_coarse_map(key, part):
    block_rows = jnp.arange(NBLK).astype(jnp.int32)
    chosen = jax.random.randint(jax.random.fold_in(key, 21), (NBLK,), 0, COARSE_DEV).astype(jnp.int32)
    return (block_rows // BLK_DEV * COARSE_DEV + chosen).astype(jnp.int32)


def draw_coupling(key, part):
    inner = jax.random.fold_in(key, 31)
    base = jax.random.normal(inner, (NCOARSE, NCOARSE), jnp.float32)
    return ((base + base.T) * (0.7071 / NCOARSE ** 0.5)).astype(jnp.float32)


def block_scale(rng, extent, split, smallest, top_value):
    def one(axis_at, blocks):
        steps = jax.random.uniform(jax.random.fold_in(jax.random.fold_in(rng, 6), axis_at), (blocks,), jnp.float32, smallest / len(split), top_value / len(split))
        return jnp.repeat(jnp.exp(steps), extent[axis_at] // blocks).reshape((-1,) + (1,) * (len(extent) - axis_at - 1))

    loudness = one(*split[0])
    for cut in split[1:]:
        loudness = loudness * one(*cut)
    return loudness


def noise(stream_key, dims, scale, reach, split=(), held_as=jnp.bfloat16):
    factor_of = block_scale(stream_key, dims, split, -0.22, 0.18) if split else 1.0
    result = jax.random.normal(stream_key, dims, jnp.float32) * scale * factor_of
    return jnp.minimum(jnp.maximum(result, -reach), reach).astype(held_as)


def setup_inputs(seed: int = 0, part: int = 0) -> dict:
    key_of = jax.random.split(jax.random.key(seed), 9)
    own_keys = jax.random.split(jax.random.fold_in(key_of[8], part), 9)
    density = noise(own_keys[0], (NBLK, RHS, BLK), 1.0, 6.0, ((0, 16),))
    near_blocks = noise(own_keys[1], (NBLK, NB, BLK, BLK), (BLK * NB) ** -0.5, 0.1875, ((0, 16),))
    neighbours = draw_neighbours(jax.random.fold_in(jax.random.fold_in(key_of[8], part), 71), part)
    counts = draw_counts(jax.random.fold_in(jax.random.fold_in(key_of[8], part), 71), part)
    coarse_map = draw_coarse_map(jax.random.fold_in(jax.random.fold_in(key_of[8], part), 71), part)
    restrict = noise(own_keys[5], (NBLK, K, BLK), (BLK * BLK_DEV // COARSE_DEV) ** -0.5, 0.125, ((0, 16),))
    evaluate = noise(own_keys[6], (NBLK, K, BLK), K ** -0.5, 0.5, ((0, 16),))
    coupling = draw_coupling(jax.random.fold_in(jax.random.fold_in(key_of[8], part), 71), part)
    return {"density": density, "near_blocks": near_blocks, "neighbours": neighbours, "counts": counts, "coarse_map": coarse_map, "restrict": restrict, "evaluate": evaluate, "coupling": coupling}


def reference(density, near_blocks, neighbours, counts, coarse_map, restrict, evaluate, coupling):
    dens_full = density.astype(jnp.float32)

    def one_block(item):
        blocks, block_ids, live_count = item
        picked = dens_full[block_ids]
        live_slots = (jnp.arange(NB).astype(jnp.int32) < live_count)[:, None, None]
        picked = jnp.where(live_slots, picked, jnp.zeros_like(picked))
        return jnp.einsum('jpq,jrq->rp', blocks.astype(jnp.float32), picked)

    near_part = lax.map(one_block, (near_blocks, neighbours, counts))
    block_terms = jnp.einsum('bkp,brp->brk', restrict.astype(jnp.float32), dens_full)
    block_terms = block_terms.reshape(NBLK, RHS * K)
    moments = jax.ops.segment_sum(block_terms, coarse_map, num_segments=NCOARSE)
    local_exp = jnp.dot(coupling, moments, precision=lax.Precision.HIGHEST).astype(jnp.bfloat16)
    spread = local_exp[coarse_map].astype(jnp.float32).reshape(NBLK, RHS, K)
    far_part = jnp.einsum('bkp,brk->brp', evaluate.astype(jnp.float32), spread)
    return (near_part + far_part).astype(jnp.bfloat16)
```

```python
import functools

import jax
import jax.numpy as jnp
from jax import lax
from jax.experimental import pallas as pl
from jax.experimental.pallas import tpu as pltpu
from jax.sharding import PartitionSpec as P

F32 = jnp.float32
BF16 = jnp.bfloat16
VMEM = pl.BlockSpec(memory_space=pltpu.VMEM)
HBM = pl.BlockSpec(memory_space=pltpu.HBM)
SMEM = pl.BlockSpec(memory_space=pltpu.SMEM)
NT = (((1,), (1,)), ((), ()))
NN = (((1,), (0,)), ((), ()))


def moments_kernel(chunks, coarse_in, density_in, restrict_in, out, kept, to_chip, to_off, coarse, restrict, sems):
    blk_count, columns, _ = density_in.shape
    groups = out.shape[0] // columns
    half = to_chip.shape[0]
    size = blk_count // chunks
    position = lax.axis_index("panel")
    odd = lax.rem(position, 2)
    first = position * groups
    copies = [
        pltpu.make_async_copy(density_in, kept, sems.at[0]),
        pltpu.make_async_copy(coarse_in, coarse, sems.at[1]),
    ]
    for i in range(chunks):
        part = pl.ds(i * size, size)
        copies.append(pltpu.make_async_copy(restrict_in.at[part], restrict.at[part], sems.at[2 + i]))
    for copy in copies:
        copy.start()
    copies[0].wait()
    to_chip[...] = kept[pl.ds((1 - odd) * half, half)]
    to_off[...] = kept[pl.ds(odd * half, half)]
    copies[1].wait()
    total = jnp.zeros(out.shape, F32)
    for b in range(0, blk_count, 2):
        if b % size == 0:
            copies[2 + b // size].wait()
        rows = []
        for c in range(groups):
            pair = []
            for i in (b, b + 1):
                here = (coarse[i] - first) == c
                block = kept[i]
                pair.append(jnp.where(here, block, jnp.zeros_like(block)))
            rows.append(jnp.concatenate(pair, axis=1))
        left = jnp.concatenate(rows, axis=0)
        right = jnp.concatenate([restrict[b], restrict[b + 1]], axis=1)
        total += lax.dot_general(left, right, NT, preferred_element_type=F32)
    out[...] = total.astype(out.dtype)


def near_kernel(begin, ids, counts, density, chip_halo, near_halo, far_halo, blocks, out, extended):
    blk_count, columns, panels = density.shape
    half = chip_halo.shape[0]
    slots = ids.shape[0]
    position = lax.axis_index("panel")
    odd = lax.rem(position, 2)
    quarter = lax.rem(position, 4)
    middle = jnp.logical_or(quarter == 1, quarter == 2)
    off_chip = jnp.where(middle, near_halo[...], far_halo[...])
    on_chip = chip_halo[...]
    extended[pl.ds(0, half)] = jnp.where(odd == 1, on_chip, off_chip)
    extended[pl.ds(half, blk_count)] = density[...]
    extended[pl.ds(half + blk_count, half)] = jnp.where(odd == 1, off_chip, on_chip)
    empty = blk_count + 2 * half
    extended[empty] = jnp.zeros((columns, panels), extended.dtype)
    shift = position * blk_count - half
    for at in range(out.shape[0]):
        b = begin + at
        live = counts[b]
        total = None
        for j in range(0, slots, 2):
            pair = []
            for i in (j, j + 1):
                slab = jnp.where(i < live, ids[i, b] - shift, empty)
                pair.append(extended[slab])
            left = jnp.concatenate(pair, axis=1)
            right = jnp.concatenate([blocks[b, j], blocks[b, j + 1]], axis=1)
            part = lax.dot_general(left, right, NT, preferred_element_type=F32)
            total = part if total is None else total + part
        out[at] = total


def weights_kernel(masks, coarse, coupling, weights, second):
    groups = coupling.shape[0]
    position = lax.axis_index("panel")
    first = position * groups
    tile = weights.shape[2:]
    for c in range(groups):
        for s, mask in enumerate(masks):
            source = lax.bitwise_xor(position, mask) * groups
            for g in range(groups):
                weights[c, s * groups + g] = jnp.full(tile, coupling[c, source + g], F32)
    for b in range(second.shape[0]):
        second[b] = jnp.full(tile, coarse[b] - first, jnp.int32)


def far_kernel(parts, weights, second, evaluate, *rest):
    moments, near, out = rest[:parts], rest[parts:-1], rest[-1]
    _, columns, panels = out.shape
    groups, _ = weights.shape[:2]
    local = []
    for c in range(groups):
        total = jnp.zeros((columns, panels), F32)
        s = 0
        for piece in moments:
            for at in range(0, piece.shape[0], columns):
                row = piece[pl.ds(at, columns)].astype(F32)
                weight = weights[c, s]
                total += row * jnp.concatenate([weight] * (columns // weight.shape[0]), axis=0)
                s += 1
        local.append(total.astype(BF16))
    left = jnp.concatenate(local, axis=0)
    begin = 0
    for part in near:
        for at in range(part.shape[0]):
            b = begin + at
            both = lax.dot_general(left, evaluate[b], NN, preferred_element_type=F32)
            pick = jnp.concatenate([second[b]] * (columns // second.shape[1]), axis=0)
            far = both[:columns]
            for c in range(1, groups):
                far = jnp.where(pick == c, both[c * columns : (c + 1) * columns], far)
            out[b] = (part[at] + far).astype(out.dtype)
        begin += part.shape[0]


def on_chip(*arrays):
    return [pltpu.with_memory_space_constraint(x, pltpu.VMEM) for x in arrays]


def in_hbm(*arrays):
    return [pltpu.with_memory_space_constraint(x, pltpu.HBM) for x in arrays]


def room(mebibytes):
    return pltpu.CompilerParams(vmem_limit_bytes=mebibytes << 20)


def cost(flops, moved):
    return pl.CostEstimate(flops=flops, bytes_accessed=moved, transcendentals=0)


def exchange(x, step):
    count = lax.axis_size("panel")
    return lax.ppermute(x, "panel", [(i, i ^ step) for i in range(count)])


def far_pairs(count):
    goes = {}
    for i in range(3, count - 1, 4):
        goes[i], goes[i + 1] = i + 1, i
    for i in range(5, count - 4, 4):
        goes[i], goes[i + 1] = i + 1, i
    for base in (0, count - 3):
        for i in range(3):
            goes[base + i] = base + (i + 1) % 3
    return sorted(goes.items())


def body(density, near_blocks, neighbours, counts, coarse_map, restrict, evaluate, coupling):
    blk_count, columns, panels = density.shape
    terms = restrict.shape[1]
    groups = coupling.shape[0]
    half = blk_count // 2
    count = lax.axis_size("panel")
    position = lax.axis_index("panel")
    odd = lax.rem(position, 2)

    steps = [(1 << bit) | 1 for bit in range(1, count.bit_length() - 1)] + [1]
    masks = [0]
    for step in steps:
        masks = masks + [mask ^ step for mask in masks]

    half_shape = (half, columns, panels)
    chunks = 4
    moments, kept, to_chip, to_off = pl.pallas_call(
        functools.partial(moments_kernel, chunks),
        out_shape=(
            pltpu.VMEM((groups * columns, terms), BF16),
            pltpu.VMEM(density.shape, BF16),
            pltpu.VMEM(half_shape, BF16),
            pltpu.VMEM(half_shape, BF16),
        ),
        in_specs=[HBM] * 3,
        out_specs=(VMEM,) * 4,
        scratch_shapes=[
            pltpu.SMEM(coarse_map.shape, jnp.int32),
            pltpu.VMEM(restrict.shape, BF16),
            pltpu.SemaphoreType.DMA((2 + chunks,)),
        ],
        compiler_params=room(8),
        cost_estimate=cost(10**10, 10**6),
        name="moments",
    )(*in_hbm(coarse_map, density, restrict))

    pieces = [moments]
    for at, step in enumerate(steps):
        sent = pieces[0] if at == 0 else jnp.concatenate(pieces, axis=0)
        pieces.append(exchange(sent, step))

    chip_halo = exchange(to_chip, 1)
    near_halo = exchange(to_off, 3)
    to_far = to_off
    far_halo = lax.ppermute(to_far, "panel", far_pairs(count))

    make_weights = pl.pallas_call(
        functools.partial(weights_kernel, masks),
        out_shape=(
            pltpu.VMEM((groups, groups * count, 8, 128), F32),
            pltpu.VMEM((blk_count, 8, 128), jnp.int32),
        ),
        in_specs=[SMEM, SMEM],
        out_specs=(VMEM, VMEM),
        compiler_params=room(4),
        cost_estimate=cost(10**11, 10**6),
        name="weights",
    )
    weights, second = make_weights(coarse_map, coupling)

    ids = neighbours.T
    near = []
    cuts = (0, 2 * blk_count // 3, blk_count)
    for begin, end in zip(cuts[:-1], cuts[1:]):
        call = (
            pl.pallas_call(
                functools.partial(near_kernel, begin),
                out_shape=pltpu.VMEM((end - begin, columns, panels), F32),
                in_specs=[SMEM, SMEM] + [VMEM] * 5,
                out_specs=VMEM,
                scratch_shapes=[pltpu.VMEM((blk_count + 2 * half + 1, columns, panels), BF16)],
                compiler_params=room(4),
                cost_estimate=cost(2 * 10**9, 10**6),
            )
        )
        near.append(call(ids, counts, *on_chip(kept, chip_halo, near_halo, far_halo, near_blocks)))

    return pl.pallas_call(
        functools.partial(far_kernel, len(pieces)),
        out_shape=jax.ShapeDtypeStruct(density.shape, BF16),
        in_specs=[VMEM] * (3 + len(pieces) + len(near)),
        out_specs=VMEM,
        compiler_params=room(4),
        cost_estimate=cost(10**9, 10**6),
        name="far",
    )(*on_chip(weights, second, evaluate, *pieces, *near))


def solution(mesh):
    placed = (
        P(("grp", "panel"), None, None),
        P(("grp", "panel"), None, None, None),
        P(("grp", "panel"), None),
        P(("grp", "panel")),
        P(("grp", "panel")),
        P(("grp", "panel"), None, None),
        P(("grp", "panel"), None, None),
        P(("grp", "panel"), None),
    )
    return jax.shard_map(
        body,
        mesh=mesh,
        in_specs=placed,
        out_specs=P(("grp", "panel"), None, None),
        check_vma=False,
    )
```

```python
import functools

import jax
import jax.numpy as jnp
from jax import lax
from jax.experimental import pallas as pl
from jax.experimental.pallas import tpu as pltpu
from jax.sharding import PartitionSpec as P

F32 = jnp.float32
BF16 = jnp.bfloat16
VMEM = pl.BlockSpec(memory_space=pltpu.VMEM)
HBM = pl.BlockSpec(memory_space=pltpu.HBM)
SMEM = pl.BlockSpec(memory_space=pltpu.SMEM)
NT = (((1,), (1,)), ((), ()))
NN = (((1,), (0,)), ((), ()))


def moments_kernel(chunks, coarse_in, density_in, restrict_in, out, kept, to_chip, to_off, coarse, restrict, masked, sems):
    blk_count, columns, panels = density_in.shape
    groups = out.shape[0] // columns
    half = to_chip.shape[0]
    size = blk_count // chunks
    position = lax.axis_index("panel")
    odd = lax.rem(position, 2)
    first = position * groups
    copies = [
        pltpu.make_async_copy(density_in, kept, sems.at[0]),
        pltpu.make_async_copy(coarse_in, coarse, sems.at[1]),
    ]
    for i in range(chunks):
        part = pl.ds(i * size, size)
        copies.append(pltpu.make_async_copy(restrict_in.at[part], restrict.at[part], sems.at[2 + i]))
    for copy in copies:
        copy.start()
    copies[0].wait()
    to_chip[...] = kept[pl.ds((1 - odd) * half, half)]
    to_off[...] = kept[pl.ds(odd * half, half)]
    copies[1].wait()
    for b in range(blk_count):
        block = kept[b]
        for c in range(groups):
            here = (coarse[b] - first) == c
            rows, lanes = slice(c * columns, (c + 1) * columns), slice(b * panels, (b + 1) * panels)
            masked[rows, lanes] = jnp.where(here, block, jnp.zeros_like(block))
    total = None
    for i in range(chunks):
        copies[2 + i].wait()
        right = jnp.concatenate([restrict[b] for b in range(i * size, (i + 1) * size)], axis=1)
        left = masked[:, i * size * panels : (i + 1) * size * panels]
        part = lax.dot_general(left, right, NT, preferred_element_type=F32)
        total = part if total is None else total + part
    out[...] = total.astype(out.dtype)


def near_kernel(on, ids, counts, density, *rest):
    halos, (blocks, out, extended) = rest[:-3], rest[-3:]
    blk_count, columns, panels = density.shape
    half = out.shape[0]
    slots = ids.shape[0]
    position = lax.axis_index("panel")
    odd = lax.rem(position, 2)
    base = (1 - odd) * half if on else odd * half
    low = odd if on else 1 - odd
    if on:
        halo = halos[0][...]
    else:
        quarter = lax.rem(position, 4)
        middle = jnp.logical_or(quarter == 1, quarter == 2)
        halo = jnp.where(middle, halos[0][...], halos[1][...])
    extended[pl.ds(half, blk_count)] = density[...]
    extended[pl.ds((1 - low) * (half + blk_count), half)] = halo
    empty = blk_count + 2 * half
    extended[empty] = jnp.zeros((columns, panels), extended.dtype)
    live = lax.broadcasted_iota(jnp.int32, ids.shape, 0) < counts[...]
    slabs = jnp.where(live, ids[...] - (position * blk_count - half), empty)
    slabs = jnp.where(base == 0, slabs[:, :half], slabs[:, half:])
    for at in range(half):
        b = base + at
        left = jnp.concatenate([extended[slabs[j, at]] for j in range(slots)], axis=1)
        right = jnp.concatenate([blocks[b, j] for j in range(slots)], axis=1)
        out[at] = lax.dot_general(left, right, NT, preferred_element_type=F32)


def weights_kernel(masks, coarse, coupling, weights, second):
    groups = coupling.shape[0]
    position = lax.axis_index("panel")
    tile = weights.shape[2:]
    columns = coupling[...]
    where_from = lax.broadcasted_iota(jnp.int32, columns.shape, 1)
    for s, mask in enumerate(masks):
        source = lax.bitwise_xor(position, mask) * groups
        for g in range(groups):
            one = jnp.sum(jnp.where(where_from == source + g, columns, 0.0), axis=1, keepdims=True)
            for c in range(groups):
                weights[c, s * groups + g] = jnp.broadcast_to(one[c : c + 1], tile)
    own = coarse[...] - position * groups
    for b in range(second.shape[0]):
        second[b] = jnp.broadcast_to(own[:, b : b + 1], tile)


def far_kernel(parts, weights, second, evaluate, *rest):
    moments, near, out = rest[:parts], rest[parts:-1], rest[-1]
    blk_count, columns, panels = out.shape
    groups, _ = weights.shape[:2]
    local = []
    for c in range(groups):
        total = jnp.zeros((columns, panels), F32)
        s = 0
        for piece in moments:
            for at in range(0, piece.shape[0], columns):
                row = piece[pl.ds(at, columns)].astype(F32)
                weight = weights[c, s]
                total += row * jnp.concatenate([weight] * (columns // weight.shape[0]), axis=0)
                s += 1
        local.append(total.astype(BF16))
    left = jnp.concatenate(local, axis=0)
    half = blk_count // 2
    odd = lax.rem(lax.axis_index("panel"), 2)
    for base, part in (((1 - odd) * half, near[0]), (odd * half, near[1])):
        for at in range(0, half, 2):
            right = jnp.concatenate([evaluate[base + at], evaluate[base + at + 1]], axis=1)
            both = lax.dot_general(left, right, NN, preferred_element_type=F32)
            for i in (0, 1):
                b = base + at + i
                pick = jnp.concatenate([second[b]] * (columns // second.shape[1]), axis=0)
                lanes = slice(i * panels, (i + 1) * panels)
                far = both[:columns, lanes]
                for c in range(1, groups):
                    far = jnp.where(pick == c, both[c * columns : (c + 1) * columns, lanes], far)
                out[b] = (part[at + i] + far).astype(out.dtype)


def on_chip(*arrays):
    return [pltpu.with_memory_space_constraint(x, pltpu.VMEM) for x in arrays]


def in_hbm(*arrays):
    return [pltpu.with_memory_space_constraint(x, pltpu.HBM) for x in arrays]


def room(mebibytes):
    return pltpu.CompilerParams(vmem_limit_bytes=mebibytes << 20)


def cost(flops, moved):
    return pl.CostEstimate(flops=flops, bytes_accessed=moved, transcendentals=0)


def exchange(x, step):
    count = lax.axis_size("panel")
    return lax.ppermute(x, "panel", [(i, i ^ step) for i in range(count)])


def far_pairs(count):
    goes = {}
    for i in range(3, count - 1, 4):
        goes[i], goes[i + 1] = i + 1, i
    for i in range(5, count - 4, 4):
        goes[i], goes[i + 1] = i + 1, i
    for base in (0, count - 3):
        for i in range(3):
            goes[base + i] = base + (i + 1) % 3
    return sorted(goes.items())


def body(density, near_blocks, neighbours, counts, coarse_map, restrict, evaluate, coupling):
    blk_count, columns, panels = density.shape
    terms = restrict.shape[1]
    groups = coupling.shape[0]
    half = blk_count // 2
    count = lax.axis_size("panel")
    position = lax.axis_index("panel")
    odd = lax.rem(position, 2)

    bits = list(range(count.bit_length() - 2, 0, -1))
    steps = [(1 << bit) | 1 for bit in bits[:1] + bits[-1:] + bits[1:-1]] + [1]
    masks = [0]
    for step in steps:
        masks = masks + [mask ^ step for mask in masks]

    half_shape = (half, columns, panels)
    chunks = 1
    moments, kept, to_chip, to_off = pl.pallas_call(
        functools.partial(moments_kernel, chunks),
        out_shape=(
            pltpu.VMEM((groups * columns, terms), BF16),
            pltpu.VMEM(density.shape, BF16),
            pltpu.VMEM(half_shape, BF16),
            pltpu.VMEM(half_shape, BF16),
        ),
        in_specs=[HBM] * 3,
        out_specs=(VMEM,) * 4,
        scratch_shapes=[
            pltpu.SMEM(coarse_map.shape, jnp.int32),
            pltpu.VMEM(restrict.shape, BF16),
            pltpu.VMEM((groups * columns, blk_count * panels), BF16),
            pltpu.SemaphoreType.DMA((2 + chunks,)),
        ],
        compiler_params=room(8),
        cost_estimate=cost(10**10, 10**6),
        name="moments",
    )(*in_hbm(coarse_map, density, restrict))

    pieces = [moments]
    for at, step in enumerate(steps):
        sent = pieces[0] if at == 0 else jnp.concatenate(pieces, axis=0)
        pieces.append(exchange(sent, step))

    chip_halo = exchange(to_chip, 1)
    near_halo = exchange(to_off, 3)
    to_far = to_off
    far_halo = lax.ppermute(to_far, "panel", far_pairs(count))

    make_weights = pl.pallas_call(
        functools.partial(weights_kernel, masks),
        out_shape=(
            pltpu.VMEM((groups, groups * count, 8, 128), F32),
            pltpu.VMEM((blk_count, 8, 128), jnp.int32),
        ),
        in_specs=[VMEM, VMEM],
        out_specs=(VMEM, VMEM),
        compiler_params=room(4),
        cost_estimate=cost(10**11, 10**6),
        name="weights",
    )
    weights, second = make_weights(*on_chip(coarse_map.reshape(1, blk_count), coupling))

    ids = neighbours.T
    live_counts = counts.reshape(1, blk_count)
    near = []
    for on, halos in ((True, (chip_halo,)), (False, (near_halo, far_halo))):
        call = pl.pallas_call(
            functools.partial(near_kernel, on),
            out_shape=pltpu.VMEM((half, columns, panels), F32),
            in_specs=[VMEM] * (4 + len(halos)),
            out_specs=VMEM,
            scratch_shapes=[
                pltpu.VMEM((blk_count + 2 * half + 1, columns, panels), BF16),
            ],
            compiler_params=room(4),
            cost_estimate=cost(2 * 10**9, 10**6),
        )
        near.append(call(*on_chip(ids, live_counts, kept, *halos, near_blocks)))

    return pl.pallas_call(
        functools.partial(far_kernel, len(pieces)),
        out_shape=jax.ShapeDtypeStruct(density.shape, BF16),
        in_specs=[VMEM] * (3 + len(pieces) + len(near)),
        out_specs=VMEM,
        compiler_params=room(4),
        cost_estimate=cost(10**9, 10**6),
        name="far",
    )(*on_chip(weights, second, evaluate, *pieces, *near))


def solution(mesh):
    placed = (
        P(("grp", "panel"), None, None),
        P(("grp", "panel"), None, None, None),
        P(("grp", "panel"), None),
        P(("grp", "panel")),
        P(("grp", "panel")),
        P(("grp", "panel"), None, None),
        P(("grp", "panel"), None, None),
        P(("grp", "panel"), None),
    )
    return jax.shard_map(
        body,
        mesh=mesh,
        in_specs=placed,
        out_specs=P(("grp", "panel"), None, None),
        check_vma=False,
    )
```

```python
import functools

import jax
import jax.numpy as jnp
from jax import lax
from jax.experimental import pallas as pl
from jax.experimental.pallas import tpu as pltpu
from jax.sharding import PartitionSpec as P

F32 = jnp.float32
BF16 = jnp.bfloat16
VMEM = pl.BlockSpec(memory_space=pltpu.VMEM)
HBM = pl.BlockSpec(memory_space=pltpu.HBM)
SMEM = pl.BlockSpec(memory_space=pltpu.SMEM)
NT = (((1,), (1,)), ((), ()))
NN = (((1,), (0,)), ((), ()))


def moments_kernel(chunks, coarse_in, density_in, restrict_in, out, kept, to_chip, to_off, coarse, restrict, masked, sems):
    blk_count, columns, panels = density_in.shape
    groups = out.shape[0] // columns
    half = to_chip.shape[0]
    size = blk_count // chunks
    position = lax.axis_index("panel")
    odd = lax.rem(position, 2)
    first = position * groups
    copies = [
        pltpu.make_async_copy(density_in, kept, sems.at[0]),
        pltpu.make_async_copy(coarse_in, coarse, sems.at[1]),
    ]
    for i in range(chunks):
        part = pl.ds(i * size, size)
        copies.append(pltpu.make_async_copy(restrict_in.at[part], restrict.at[part], sems.at[2 + i]))
    for copy in copies:
        copy.start()
    copies[0].wait()
    to_chip[...] = kept[pl.ds((1 - odd) * half, half)]
    to_off[...] = kept[pl.ds(odd * half, half)]
    copies[1].wait()
    for b in range(blk_count):
        block = kept[b]
        for c in range(groups):
            here = (coarse[b] - first) == c
            rows, lanes = slice(c * columns, (c + 1) * columns), slice(b * panels, (b + 1) * panels)
            masked[rows, lanes] = jnp.where(here, block, jnp.zeros_like(block))
    total = None
    for i in range(chunks):
        copies[2 + i].wait()
        right = jnp.concatenate([restrict[b] for b in range(i * size, (i + 1) * size)], axis=1)
        left = masked[:, i * size * panels : (i + 1) * size * panels]
        part = lax.dot_general(left, right, NT, preferred_element_type=F32)
        total = part if total is None else total + part
    out[...] = total.astype(out.dtype)


def near_kernel(on, begin, ids, counts, density, *rest):
    halos, (blocks, out, extended) = rest[:-3], rest[-3:]
    blk_count, columns, panels = density.shape
    half = halos[0].shape[0]
    slots = ids.shape[0]
    position = lax.axis_index("panel")
    odd = lax.rem(position, 2)
    base = (1 - odd) * half if on else odd * half
    low = odd if on else 1 - odd
    if on:
        halo = halos[0][...]
    else:
        relayed = jnp.logical_or(position == 1, position == lax.axis_size("panel") - 2)
        halo = jnp.where(relayed, halos[1][...], halos[0][...])
    extended[pl.ds(half, blk_count)] = density[...]
    extended[pl.ds((1 - low) * (half + blk_count), half)] = halo
    empty = blk_count + 2 * half
    extended[empty] = jnp.zeros((columns, panels), extended.dtype)
    live = lax.broadcasted_iota(jnp.int32, ids.shape, 0) < counts[...]
    slabs = jnp.where(live, ids[...] - (position * blk_count - half), empty)
    slabs = jnp.where(base == 0, slabs[:, :half], slabs[:, half:])
    for at in range(out.shape[0]):
        b = base + begin + at
        left = [extended[slabs[j, begin + at]] for j in range(slots)]
        mid = slots // 2
        turned = jnp.concatenate([blocks[b, j].T for j in range(mid)], axis=0)
        plain = jnp.concatenate([blocks[b, j] for j in range(mid, slots)], axis=1)
        out[at] = lax.dot_general(
            jnp.concatenate(left[mid:], axis=1), plain, NT, preferred_element_type=F32
        ) + lax.dot_general(jnp.concatenate(left[:mid], axis=1), turned, NN, preferred_element_type=F32)


def weights_kernel(masks, coarse, coupling, mark, weights, second):
    groups = coupling.shape[0]
    position = lax.axis_index("panel")
    tile = weights.shape[2:]
    columns = coupling[...]
    where_from = lax.broadcasted_iota(jnp.int32, columns.shape, 1)
    for s, mask in enumerate(masks):
        source = lax.bitwise_xor(position, mask) * groups
        for g in range(groups):
            one = jnp.sum(jnp.where(where_from == source + g, columns, 0.0), axis=1, keepdims=True)
            for c in range(groups):
                weights[c, s * groups + g] = jnp.broadcast_to(one[c : c + 1], tile)
    own = coarse[...] - position * groups
    for b in range(second.shape[0]):
        second[b] = jnp.broadcast_to(own[:, b : b + 1], tile)


def mark_kernel(out):
    out[...] = jnp.zeros_like(out)


def far_kernel(cuts, parts, weights, second, evaluate, *rest):
    moments, near, out = rest[:parts], rest[parts:-1], rest[-1]
    blk_count, columns, panels = out.shape
    groups, _ = weights.shape[:2]
    local = []
    for c in range(groups):
        total = jnp.zeros((columns, panels), F32)
        s = 0
        for piece in moments:
            for at in range(0, piece.shape[0], columns):
                row = piece[pl.ds(at, columns)].astype(F32)
                weight = weights[c, s]
                total += row * jnp.concatenate([weight] * (columns // weight.shape[0]), axis=0)
                s += 1
        local.append(total.astype(BF16))
    left = jnp.concatenate(local, axis=0)
    half = blk_count // 2
    odd = lax.rem(lax.axis_index("panel"), 2)
    for (on, begin, end), part in zip(cuts, near):
        base = ((1 - odd) * half if on else odd * half) + begin
        for at in range(0, end - begin, 2):
            right = jnp.concatenate([evaluate[base + at], evaluate[base + at + 1]], axis=1)
            both = lax.dot_general(left, right, NN, preferred_element_type=F32)
            for i in (0, 1):
                b = base + at + i
                pick = jnp.concatenate([second[b]] * (columns // second.shape[1]), axis=0)
                lanes = slice(i * panels, (i + 1) * panels)
                far = both[:columns, lanes]
                for c in range(1, groups):
                    far = jnp.where(pick == c, both[c * columns : (c + 1) * columns, lanes], far)
                out[b] = (part[at + i] + far).astype(out.dtype)


def on_chip(*arrays):
    return [pltpu.with_memory_space_constraint(x, pltpu.VMEM) for x in arrays]


def in_hbm(*arrays):
    return [pltpu.with_memory_space_constraint(x, pltpu.HBM) for x in arrays]


def room(mebibytes):
    return pltpu.CompilerParams(vmem_limit_bytes=mebibytes << 20)


def cost(flops, moved):
    return pl.CostEstimate(flops=flops, bytes_accessed=moved, transcendentals=0)


def exchange(x, step):
    count = lax.axis_size("panel")
    return lax.ppermute(x, "panel", [(i, i ^ step) for i in range(count)])


def off_pairs(count):
    goes = {0: 1, 1: 2, 2: 0, count - 3: count - 1, count - 1: count - 2, count - 2: count - 3}
    for i in range(3, count - 4, 2):
        goes[i], goes[i + 1] = i + 1, i
    return sorted(goes.items())


def body(density, near_blocks, neighbours, counts, coarse_map, restrict, evaluate, coupling):
    blk_count, columns, panels = density.shape
    terms = restrict.shape[1]
    groups = coupling.shape[0]
    half = blk_count // 2
    count = lax.axis_size("panel")
    position = lax.axis_index("panel")
    odd = lax.rem(position, 2)

    rounds = rounds_of(count)
    masks = [0]
    for together in rounds:
        masks = masks + [mask ^ step for step in together for mask in masks]

    half_shape = (half, columns, panels)
    chunks = 1
    moments, kept, to_chip, to_off = pl.pallas_call(
        functools.partial(moments_kernel, chunks),
        out_shape=(
            pltpu.VMEM((groups * columns, terms), BF16),
            pltpu.VMEM(density.shape, BF16),
            pltpu.VMEM(half_shape, BF16),
            pltpu.VMEM(half_shape, BF16),
        ),
        in_specs=[HBM] * 3,
        out_specs=(VMEM,) * 4,
        scratch_shapes=[
            pltpu.SMEM(coarse_map.shape, jnp.int32),
            pltpu.VMEM(restrict.shape, BF16),
            pltpu.VMEM((groups * columns, blk_count * panels), BF16),
            pltpu.SemaphoreType.DMA((2 + chunks,)),
        ],
        compiler_params=room(8),
        cost_estimate=cost(10**10, 10**6),
        name="moments",
    )(*in_hbm(coarse_map, density, restrict))

    pieces = [moments]
    for at, together in enumerate(rounds):
        sent = pieces[0] if at == 0 else jnp.concatenate(pieces, axis=0)
        for step in together:
            pieces.append(exchange(sent, step))

    chip_halo = exchange(to_chip, 1)
    off_halo = lax.ppermute(to_off, "panel", off_pairs(count))
    relay = exchange(off_halo, 1)

    make_mark = pl.pallas_call(
        mark_kernel,
        out_shape=pltpu.VMEM((8, 128), F32),
        out_specs=VMEM,
        compiler_params=room(1),
        cost_estimate=cost(10**11, 10**6),
        name="mark",
    )
    mark = make_mark()
    make_weights = pl.pallas_call(
        functools.partial(weights_kernel, masks),
        out_shape=(
            pltpu.VMEM((groups, groups * count, 8, 128), F32),
            pltpu.VMEM((blk_count, 8, 128), jnp.int32),
        ),
        in_specs=[VMEM] * 3,
        out_specs=(VMEM, VMEM),
        compiler_params=room(4),
        cost_estimate=cost(10**9, 10**6),
        name="weights",
    )
    weights, second = make_weights(*on_chip(coarse_map.reshape(1, blk_count), coupling, mark))

    ids = neighbours.T
    live_counts = counts.reshape(1, blk_count)
    near = []
    cuts = [(on, begin * half // 8, end * half // 8) for on, begin, end in CUTS]
    for on, begin, end in cuts:
        halos = (chip_halo,) if on else (off_halo, relay)
        call = pl.pallas_call(
            functools.partial(near_kernel, on, begin),
            out_shape=pltpu.VMEM((end - begin, columns, panels), F32),
            in_specs=[VMEM] * (4 + len(halos)),
            out_specs=VMEM,
            scratch_shapes=[
                pltpu.VMEM((blk_count + 2 * half + 1, columns, panels), BF16),
            ],
            compiler_params=room(4),
            cost_estimate=cost(2 * 10**9, 10**6),
        )
        near.append(call(*on_chip(ids, live_counts, kept, *halos, near_blocks)))

    return pl.pallas_call(
        functools.partial(far_kernel, cuts, len(pieces)),
        out_shape=jax.ShapeDtypeStruct(density.shape, BF16),
        in_specs=[VMEM] * (3 + len(pieces) + len(near)),
        out_specs=VMEM,
        compiler_params=room(4),
        cost_estimate=cost(10**9, 10**6),
        name="far",
    )(*on_chip(weights, second, evaluate, *pieces, *near))


CUTS = ((True, 0, 8), (False, 0, 3), (False, 3, 8))


def rounds_of(count):
    return [[(1 << bit) | 1] for bit in range(count.bit_length() - 2, 2, -1)] + [[6, 3, 5], [1]]


def solution(mesh):
    placed = (
        P(("grp", "panel"), None, None),
        P(("grp", "panel"), None, None, None),
        P(("grp", "panel"), None),
        P(("grp", "panel")),
        P(("grp", "panel")),
        P(("grp", "panel"), None, None),
        P(("grp", "panel"), None, None),
        P(("grp", "panel"), None),
    )
    return jax.shard_map(
        body,
        mesh=mesh,
        in_specs=placed,
        out_specs=P(("grp", "panel"), None, None),
        check_vma=False,
    )
```

```python
import functools

import jax
import jax.numpy as jnp
from jax import lax
from jax.experimental import pallas as pl
from jax.experimental.pallas import tpu as pltpu
from jax.sharding import PartitionSpec as P

F32 = jnp.float32
BF16 = jnp.bfloat16
VMEM = pl.BlockSpec(memory_space=pltpu.VMEM)
HBM = pl.BlockSpec(memory_space=pltpu.HBM)
SMEM = pl.BlockSpec(memory_space=pltpu.SMEM)
NT = (((1,), (1,)), ((), ()))
NN = (((1,), (0,)), ((), ()))


def moments_kernel(chunks, coarse_in, density_in, restrict_in, out, kept, to_chip, to_off, coarse, restrict, masked, sems):
    blk_count, columns, panels = density_in.shape
    groups = out.shape[0] // columns
    half = to_chip.shape[0]
    size = blk_count // chunks
    position = lax.axis_index("panel")
    odd = lax.rem(position, 2)
    first = position * groups
    copies = [
        pltpu.make_async_copy(density_in, kept, sems.at[0]),
        pltpu.make_async_copy(coarse_in, coarse, sems.at[1]),
    ]
    for i in range(chunks):
        part = pl.ds(i * size, size)
        copies.append(pltpu.make_async_copy(restrict_in.at[part], restrict.at[part], sems.at[2 + i]))
    for copy in copies:
        copy.start()
    copies[0].wait()
    to_chip[...] = kept[pl.ds((1 - odd) * half, half)]
    to_off[...] = kept[pl.ds(odd * half, half)]
    copies[1].wait()
    for b in range(blk_count):
        block = kept[b]
        for c in range(groups):
            here = (coarse[b] - first) == c
            rows, lanes = slice(c * columns, (c + 1) * columns), slice(b * panels, (b + 1) * panels)
            masked[rows, lanes] = jnp.where(here, block, jnp.zeros_like(block))
    for copy in copies[2:]:
        copy.wait()
    right = jnp.concatenate([restrict[b] for b in range(blk_count)], axis=1)
    out[...] = lax.dot_general(masked[...], right, NT, preferred_element_type=F32).astype(out.dtype)


def near_kernel(on, begin, ids, counts, density, *rest):
    halos, (blocks, out, extended) = rest[:-3], rest[-3:]
    blk_count, columns, panels = density.shape
    half = halos[0].shape[0]
    slots = ids.shape[0]
    position = lax.axis_index("panel")
    odd = lax.rem(position, 2)
    base = (1 - odd) * half if on else odd * half
    low = odd if on else 1 - odd
    if on:
        halo = halos[0][...]
    else:
        relayed = jnp.logical_or(position == 1, position == lax.axis_size("panel") - 2)
        halo = jnp.where(relayed, halos[1][...], halos[0][...])
    extended[pl.ds(half, blk_count)] = density[...]
    extended[pl.ds((1 - low) * (half + blk_count), half)] = halo
    empty = blk_count + 2 * half
    extended[empty] = jnp.zeros((columns, panels), extended.dtype)
    live = lax.broadcasted_iota(jnp.int32, ids.shape, 0) < counts[...]
    slabs = jnp.where(live, ids[...] - (position * blk_count - half), empty)
    slabs = jnp.where(base == 0, slabs[:, :half], slabs[:, half:])
    for at in range(out.shape[0]):
        b = base + begin + at
        left = [extended[slabs[j, begin + at]] for j in range(slots)]
        mid = slots // 2
        turned = jnp.concatenate([blocks[b, j].T for j in range(mid)], axis=0)
        plain = jnp.concatenate([blocks[b, j] for j in range(mid, slots)], axis=1)
        out[at] = lax.dot_general(
            jnp.concatenate(left[mid:], axis=1), plain, NT, preferred_element_type=F32
        ) + lax.dot_general(jnp.concatenate(left[:mid], axis=1), turned, NN, preferred_element_type=F32)


def weights_kernel(masks, coarse, coupling, mark, weights, second):
    groups = coupling.shape[0]
    position = lax.axis_index("panel")
    tile = weights.shape[2:]
    columns = coupling[...]
    where_from = lax.broadcasted_iota(jnp.int32, columns.shape, 1)
    for s, mask in enumerate(masks):
        source = lax.bitwise_xor(position, mask) * groups
        for g in range(groups):
            one = jnp.sum(jnp.where(where_from == source + g, columns, 0.0), axis=1, keepdims=True)
            for c in range(groups):
                weights[c, s * groups + g] = jnp.broadcast_to(one[c : c + 1], tile)
    own = coarse[...] - position * groups
    for b in range(second.shape[0]):
        second[b] = jnp.broadcast_to(own[:, b : b + 1], tile)


def mark_kernel(out):
    out[...] = jnp.zeros_like(out)


def far_kernel(cuts, parts, weights, second, evaluate, *rest):
    moments, near, out = rest[:parts], rest[parts:-1], rest[-1]
    blk_count, columns, panels = out.shape
    groups, _ = weights.shape[:2]
    local = []
    for c in range(groups):
        terms = []
        for piece in moments:
            for at in range(0, piece.shape[0], columns):
                row = piece[pl.ds(at, columns)].astype(F32)
                weight = weights[c, len(terms)]
                terms.append(row * jnp.concatenate([weight] * (columns // weight.shape[0]), axis=0))
        while len(terms) > 1:
            half_terms = len(terms) // 2
            terms = [terms[i] + terms[i + half_terms] for i in range(half_terms)] + terms[2 * half_terms :]
        local.append(terms[0].astype(BF16))
    left = jnp.concatenate(local, axis=0)
    half = blk_count // 2
    odd = lax.rem(lax.axis_index("panel"), 2)
    for (on, begin, end), part in zip(cuts, near):
        base = ((1 - odd) * half if on else odd * half) + begin
        for at in range(0, end - begin, 2):
            right = jnp.concatenate([evaluate[base + at], evaluate[base + at + 1]], axis=1)
            both = lax.dot_general(left, right, NN, preferred_element_type=F32)
            for i in (0, 1):
                b = base + at + i
                pick = jnp.concatenate([second[b]] * (columns // second.shape[1]), axis=0)
                lanes = slice(i * panels, (i + 1) * panels)
                far = both[:columns, lanes]
                for c in range(1, groups):
                    far = jnp.where(pick == c, both[c * columns : (c + 1) * columns, lanes], far)
                out[b] = (part[at + i] + far).astype(out.dtype)


def on_chip(*arrays):
    return [pltpu.with_memory_space_constraint(x, pltpu.VMEM) for x in arrays]


def in_hbm(*arrays):
    return [pltpu.with_memory_space_constraint(x, pltpu.HBM) for x in arrays]


def room(mebibytes):
    return pltpu.CompilerParams(vmem_limit_bytes=mebibytes << 20)


def cost(flops, moved):
    return pl.CostEstimate(flops=flops, bytes_accessed=moved, transcendentals=0)


def exchange(x, step):
    count = lax.axis_size("panel")
    return lax.ppermute(x, "panel", [(i, i ^ step) for i in range(count)])


def off_pairs(count):
    goes = {0: 1, 1: 2, 2: 0, count - 3: count - 1, count - 1: count - 2, count - 2: count - 3}
    for i in range(3, count - 4, 2):
        goes[i], goes[i + 1] = i + 1, i
    return sorted(goes.items())


def body(density, near_blocks, neighbours, counts, coarse_map, restrict, evaluate, coupling):
    blk_count, columns, panels = density.shape
    terms = restrict.shape[1]
    groups = coupling.shape[0]
    half = blk_count // 2
    count = lax.axis_size("panel")
    position = lax.axis_index("panel")
    odd = lax.rem(position, 2)

    rounds = rounds_of(count)
    masks = [0]
    for together in rounds:
        masks = masks + [mask ^ step for step in together for mask in masks]

    half_shape = (half, columns, panels)
    chunks = 4
    moments, kept, to_chip, to_off = pl.pallas_call(
        functools.partial(moments_kernel, chunks),
        out_shape=(
            pltpu.VMEM((groups * columns, terms), BF16),
            pltpu.VMEM(density.shape, BF16),
            pltpu.VMEM(half_shape, BF16),
            pltpu.VMEM(half_shape, BF16),
        ),
        in_specs=[HBM] * 3,
        out_specs=(VMEM,) * 4,
        scratch_shapes=[
            pltpu.SMEM(coarse_map.shape, jnp.int32),
            pltpu.VMEM(restrict.shape, BF16),
            pltpu.VMEM((groups * columns, blk_count * panels), BF16),
            pltpu.SemaphoreType.DMA((2 + chunks,)),
        ],
        compiler_params=room(8),
        cost_estimate=cost(10**10, 10**6),
        name="moments",
    )(*in_hbm(coarse_map, density, restrict))

    pieces = [moments]
    for at, together in enumerate(rounds):
        sent = pieces[0] if at == 0 else jnp.concatenate(pieces, axis=0)
        for step in together:
            pieces.append(exchange(sent, step))

    chip_halo = exchange(to_chip, 1)
    off_halo = lax.ppermute(to_off, "panel", off_pairs(count))
    relay = exchange(off_halo, 1)

    make_mark = pl.pallas_call(
        mark_kernel,
        out_shape=pltpu.VMEM((8, 128), F32),
        out_specs=VMEM,
        compiler_params=room(1),
        cost_estimate=cost(10**11, 10**6),
        name="mark",
    )
    mark = make_mark()
    make_weights = pl.pallas_call(
        functools.partial(weights_kernel, masks),
        out_shape=(
            pltpu.VMEM((groups, groups * count, 8, 128), F32),
            pltpu.VMEM((blk_count, 8, 128), jnp.int32),
        ),
        in_specs=[VMEM] * 3,
        out_specs=(VMEM, VMEM),
        compiler_params=room(4),
        cost_estimate=cost(10**9, 10**6),
        name="weights",
    )
    weights, second = make_weights(*on_chip(coarse_map.reshape(1, blk_count), coupling, mark))

    ids = neighbours.T
    live_counts = counts.reshape(1, blk_count)
    near = []
    cuts = [(on, begin * half // 8, end * half // 8) for on, begin, end in CUTS]
    for on, begin, end in cuts:
        halos = (chip_halo,) if on else (off_halo, relay)
        call = pl.pallas_call(
            functools.partial(near_kernel, on, begin),
            out_shape=pltpu.VMEM((end - begin, columns, panels), F32),
            in_specs=[VMEM] * (4 + len(halos)),
            out_specs=VMEM,
            scratch_shapes=[
                pltpu.VMEM((blk_count + 2 * half + 1, columns, panels), BF16),
            ],
            compiler_params=room(4),
            cost_estimate=cost(2 * 10**9, 10**6),
        )
        near.append(call(*on_chip(ids, live_counts, kept, *halos, near_blocks)))

    return pl.pallas_call(
        functools.partial(far_kernel, cuts, len(pieces)),
        out_shape=jax.ShapeDtypeStruct(density.shape, BF16),
        in_specs=[VMEM] * (3 + len(pieces) + len(near)),
        out_specs=VMEM,
        compiler_params=room(4),
        cost_estimate=cost(10**9, 10**6),
        name="far",
    )(*on_chip(weights, second, evaluate, *pieces, *near))


CUTS = ((True, 0, 8), (False, 0, 4), (False, 4, 8))


def rounds_of(count):
    return [[(1 << bit) | 1] for bit in range(count.bit_length() - 2, 2, -1)] + [[7, 5, 3], [1]]


def solution(mesh):
    placed = (
        P(("grp", "panel"), None, None),
        P(("grp", "panel"), None, None, None),
        P(("grp", "panel"), None),
        P(("grp", "panel")),
        P(("grp", "panel")),
        P(("grp", "panel"), None, None),
        P(("grp", "panel"), None, None),
        P(("grp", "panel"), None),
    )
    return jax.shard_map(
        body,
        mesh=mesh,
        in_specs=placed,
        out_specs=P(("grp", "panel"), None, None),
        check_vma=False,
    )
```

```python
import functools

import jax
import jax.numpy as jnp
from jax import lax
from jax.experimental import pallas as pl
from jax.experimental.pallas import tpu as pltpu
from jax.sharding import PartitionSpec as P

F32 = jnp.float32
BF16 = jnp.bfloat16
VMEM = pl.BlockSpec(memory_space=pltpu.VMEM)
HBM = pl.BlockSpec(memory_space=pltpu.HBM)
SMEM = pl.BlockSpec(memory_space=pltpu.SMEM)
NT = (((1,), (1,)), ((), ()))
NN = (((1,), (0,)), ((), ()))


def moments_kernel(chunks, coarse_in, density_in, restrict_in, out, kept, to_chip, to_off, coarse, restrict, masked, sems):
    blk_count, columns, panels = density_in.shape
    groups = out.shape[0] // columns
    half = to_chip.shape[0]
    size = blk_count // chunks
    position = lax.axis_index("panel")
    odd = lax.rem(position, 2)
    first = position * groups
    copies = [
        pltpu.make_async_copy(density_in, kept, sems.at[0]),
        pltpu.make_async_copy(coarse_in, coarse, sems.at[1]),
    ]
    for i in range(chunks):
        part = pl.ds(i * size, size)
        copies.append(pltpu.make_async_copy(restrict_in.at[part], restrict.at[part], sems.at[2 + i]))
    for copy in copies:
        copy.start()
    copies[0].wait()
    to_chip[...] = kept[pl.ds((1 - odd) * half, half)]
    to_off[...] = kept[pl.ds(odd * half, half)]
    copies[1].wait()
    for b in range(blk_count):
        block = kept[b]
        for c in range(groups):
            here = (coarse[b] - first) == c
            rows, lanes = slice(c * columns, (c + 1) * columns), slice(b * panels, (b + 1) * panels)
            masked[rows, lanes] = jnp.where(here, block, jnp.zeros_like(block))
    for copy in copies[2:]:
        copy.wait()
    right = jnp.concatenate([restrict[b] for b in range(blk_count)], axis=1)
    out[...] = lax.dot_general(masked[...], right, NT, preferred_element_type=F32).astype(out.dtype)


def near_kernel(on, begin, ids, counts, density, *rest):
    halos, (blocks, out, extended) = rest[:-3], rest[-3:]
    blk_count, columns, panels = density.shape
    half = halos[0].shape[0]
    slots = ids.shape[0]
    position = lax.axis_index("panel")
    odd = lax.rem(position, 2)
    base = (1 - odd) * half if on else odd * half
    low = odd if on else 1 - odd
    if on:
        halo = halos[0][...]
    else:
        relayed = jnp.logical_or(position == 1, position == lax.axis_size("panel") - 2)
        halo = jnp.where(relayed, halos[1][...], halos[0][...])
    extended[pl.ds(half, blk_count)] = density[...]
    extended[pl.ds((1 - low) * (half + blk_count), half)] = halo
    empty = blk_count + 2 * half
    extended[empty] = jnp.zeros((columns, panels), extended.dtype)
    live = lax.broadcasted_iota(jnp.int32, ids.shape, 0) < counts[...]
    slabs = jnp.where(live, ids[...] - (position * blk_count - half), empty)
    slabs = jnp.where(base == 0, slabs[:, :half], slabs[:, half:])
    for at in range(out.shape[0]):
        b = base + begin + at
        left = [extended[slabs[j, begin + at]] for j in range(slots)]
        mid = slots // 2
        turned = jnp.concatenate([blocks[b, j].T for j in range(mid)], axis=0)
        plain = jnp.concatenate([blocks[b, j] for j in range(mid, slots)], axis=1)
        out[at] = lax.dot_general(
            jnp.concatenate(left[mid:], axis=1), plain, NT, preferred_element_type=F32
        ) + lax.dot_general(jnp.concatenate(left[:mid], axis=1), turned, NN, preferred_element_type=F32)


def weights_kernel(masks, coarse, coupling, mark, weights, second):
    groups = coupling.shape[0]
    position = lax.axis_index("panel")
    tile = weights.shape[2:]
    columns = coupling[...]
    where_from = lax.broadcasted_iota(jnp.int32, columns.shape, 1)
    for s, mask in enumerate(masks):
        source = lax.bitwise_xor(position, mask) * groups
        for g in range(groups):
            one = jnp.sum(jnp.where(where_from == source + g, columns, 0.0), axis=1, keepdims=True)
            for c in range(groups):
                weights[c, s * groups + g] = jnp.broadcast_to(one[c : c + 1], tile)
    own = coarse[...] - position * groups
    for b in range(second.shape[0]):
        second[b] = jnp.broadcast_to(own[:, b : b + 1], tile)


def mark_kernel(out):
    out[...] = jnp.zeros_like(out)


def coupled(pieces, weights, c, first, columns):
    terms = []
    for piece in pieces:
        for at in range(0, piece.shape[0], columns):
            row = piece[pl.ds(at, columns)].astype(F32)
            weight = weights[c, first + len(terms)]
            terms.append(row * jnp.concatenate([weight] * (columns // weight.shape[0]), axis=0))
    while len(terms) > 1:
        half = len(terms) // 2
        terms = [terms[i] + terms[i + half] for i in range(half)] + terms[2 * half :]
    return terms[0]


def partial_kernel(weights, *rest):
    pieces, out = rest[:-1], rest[-1]
    for c in range(out.shape[0]):
        out[c] = coupled(pieces, weights, c, 0, out.shape[1])


def far_kernel(cuts, weights, second, evaluate, known, last, *rest):
    near, out = rest[:-1], rest[-1]
    blk_count, columns, panels = out.shape
    groups, slots = weights.shape[:2]
    local = []
    for c in range(groups):
        total = known[c] + coupled((last,), weights, c, slots - last.shape[0] // columns, columns)
        local.append(total.astype(BF16))
    left = jnp.concatenate(local, axis=0)
    half = blk_count // 2
    odd = lax.rem(lax.axis_index("panel"), 2)
    for (on, begin, end), part in zip(cuts, near):
        base = ((1 - odd) * half if on else odd * half) + begin
        for at in range(0, end - begin, 2):
            right = jnp.concatenate([evaluate[base + at], evaluate[base + at + 1]], axis=1)
            both = lax.dot_general(left, right, NN, preferred_element_type=F32)
            for i in (0, 1):
                b = base + at + i
                pick = jnp.concatenate([second[b]] * (columns // second.shape[1]), axis=0)
                lanes = slice(i * panels, (i + 1) * panels)
                far = both[:columns, lanes]
                for c in range(1, groups):
                    far = jnp.where(pick == c, both[c * columns : (c + 1) * columns, lanes], far)
                out[b] = (part[at + i] + far).astype(out.dtype)


def on_chip(*arrays):
    return [pltpu.with_memory_space_constraint(x, pltpu.VMEM) for x in arrays]


def in_hbm(*arrays):
    return [pltpu.with_memory_space_constraint(x, pltpu.HBM) for x in arrays]


def room(mebibytes):
    return pltpu.CompilerParams(vmem_limit_bytes=mebibytes << 20)


def cost(flops, moved):
    return pl.CostEstimate(flops=flops, bytes_accessed=moved, transcendentals=0)


def exchange(x, step):
    count = lax.axis_size("panel")
    return lax.ppermute(x, "panel", [(i, i ^ step) for i in range(count)])


def off_pairs(count):
    goes = {0: 1, 1: 2, 2: 0, count - 3: count - 1, count - 1: count - 2, count - 2: count - 3}
    for i in range(3, count - 4, 2):
        goes[i], goes[i + 1] = i + 1, i
    return sorted(goes.items())


def body(density, near_blocks, neighbours, counts, coarse_map, restrict, evaluate, coupling):
    blk_count, columns, panels = density.shape
    terms = restrict.shape[1]
    groups = coupling.shape[0]
    half = blk_count // 2
    count = lax.axis_size("panel")
    position = lax.axis_index("panel")
    odd = lax.rem(position, 2)

    rounds = rounds_of(count)
    masks = [0]
    for together in rounds:
        masks = masks + [mask ^ step for step in together for mask in masks]

    half_shape = (half, columns, panels)
    chunks = 4
    moments, kept, to_chip, to_off = pl.pallas_call(
        functools.partial(moments_kernel, chunks),
        out_shape=(
            pltpu.VMEM((groups * columns, terms), BF16),
            pltpu.VMEM(density.shape, BF16),
            pltpu.VMEM(half_shape, BF16),
            pltpu.VMEM(half_shape, BF16),
        ),
        in_specs=[HBM] * 3,
        out_specs=(VMEM,) * 4,
        scratch_shapes=[
            pltpu.SMEM(coarse_map.shape, jnp.int32),
            pltpu.VMEM(restrict.shape, BF16),
            pltpu.VMEM((groups * columns, blk_count * panels), BF16),
            pltpu.SemaphoreType.DMA((2 + chunks,)),
        ],
        compiler_params=room(8),
        cost_estimate=cost(10**10, 10**6),
        name="moments",
    )(*in_hbm(coarse_map, density, restrict))

    pieces = [moments]
    for at, together in enumerate(rounds):
        sent = pieces[0] if at == 0 else jnp.concatenate(pieces, axis=0)
        for step in together:
            pieces.append(exchange(sent, step))

    chip_halo = exchange(to_chip, 1)
    off_halo = lax.ppermute(to_off, "panel", off_pairs(count))
    relay = exchange(off_halo, 1)

    make_mark = pl.pallas_call(
        mark_kernel,
        out_shape=pltpu.VMEM((8, 128), F32),
        out_specs=VMEM,
        compiler_params=room(1),
        cost_estimate=cost(10**11, 10**6),
        name="mark",
    )
    mark = make_mark()
    make_weights = pl.pallas_call(
        functools.partial(weights_kernel, masks),
        out_shape=(
            pltpu.VMEM((groups, groups * count, 8, 128), F32),
            pltpu.VMEM((blk_count, 8, 128), jnp.int32),
        ),
        in_specs=[VMEM] * 3,
        out_specs=(VMEM, VMEM),
        compiler_params=room(4),
        cost_estimate=cost(10**9, 10**6),
        name="weights",
    )
    weights, second = make_weights(*on_chip(coarse_map.reshape(1, blk_count), coupling, mark))

    ids = neighbours.T
    live_counts = counts.reshape(1, blk_count)
    near = []
    cuts = [(on, begin * half // 8, end * half // 8) for on, begin, end in CUTS]
    for on, begin, end in cuts:
        halos = (chip_halo,) if on else (off_halo, relay)
        call = pl.pallas_call(
            functools.partial(near_kernel, on, begin),
            out_shape=pltpu.VMEM((end - begin, columns, panels), F32),
            in_specs=[VMEM] * (4 + len(halos)),
            out_specs=VMEM,
            scratch_shapes=[
                pltpu.VMEM((blk_count + 2 * half + 1, columns, panels), BF16),
            ],
            compiler_params=room(4),
            cost_estimate=cost(2 * 10**9, 10**6),
        )
        near.append(call(*on_chip(ids, live_counts, kept, *halos, near_blocks)))

    make_partial = pl.pallas_call(
        partial_kernel,
        out_shape=pltpu.VMEM((groups, columns, panels), F32),
        in_specs=[VMEM] * len(pieces),
        out_specs=VMEM,
        compiler_params=room(4),
        cost_estimate=cost(10**9, 10**6),
        name="partial",
    )
    known = make_partial(*on_chip(weights, *pieces[:-1]))

    return pl.pallas_call(
        functools.partial(far_kernel, cuts),
        out_shape=jax.ShapeDtypeStruct(density.shape, BF16),
        in_specs=[VMEM] * (5 + len(near)),
        out_specs=VMEM,
        compiler_params=room(4),
        cost_estimate=cost(10**9, 10**6),
        name="far",
    )(*on_chip(weights, second, evaluate, known, pieces[-1], *near))


CUTS = ((True, 0, 8), (False, 0, 4), (False, 4, 8))


def rounds_of(count):
    return [[(1 << bit) | 1] for bit in range(count.bit_length() - 2, 2, -1)] + [[7, 5, 3], [1]]


def solution(mesh):
    placed = (
        P(("grp", "panel"), None, None),
        P(("grp", "panel"), None, None, None),
        P(("grp", "panel"), None),
        P(("grp", "panel")),
        P(("grp", "panel")),
        P(("grp", "panel"), None, None),
        P(("grp", "panel"), None, None),
        P(("grp", "panel"), None),
    )
    return jax.shard_map(
        body,
        mesh=mesh,
        in_specs=placed,
        out_specs=P(("grp", "panel"), None, None),
        check_vma=False,
    )
```

```python
import functools

import jax
import jax.numpy as jnp
from jax import lax
from jax.experimental import pallas as pl
from jax.experimental.pallas import tpu as pltpu
from jax.sharding import PartitionSpec as P

F32 = jnp.float32
BF16 = jnp.bfloat16
VMEM = pl.BlockSpec(memory_space=pltpu.VMEM)
HBM = pl.BlockSpec(memory_space=pltpu.HBM)
SMEM = pl.BlockSpec(memory_space=pltpu.SMEM)
NT = (((1,), (1,)), ((), ()))
NN = (((1,), (0,)), ((), ()))


def moments_kernel(chunks, coarse_in, density_in, restrict_in, out, kept, to_chip, to_off, coarse, restrict, masked, sems):
    blk_count, columns, panels = density_in.shape
    groups = out.shape[0] // columns
    half = to_chip.shape[0]
    size = blk_count // chunks
    position = lax.axis_index("panel")
    odd = lax.rem(position, 2)
    first = position * groups
    copies = [
        pltpu.make_async_copy(density_in, kept, sems.at[0]),
        pltpu.make_async_copy(coarse_in, coarse, sems.at[1]),
    ]
    for i in range(chunks):
        part = pl.ds(i * size, size)
        copies.append(pltpu.make_async_copy(restrict_in.at[part], restrict.at[part], sems.at[2 + i]))
    for copy in copies:
        copy.start()
    copies[0].wait()
    to_chip[...] = kept[pl.ds((1 - odd) * half, half)]
    to_off[...] = kept[pl.ds(odd * half, half)]
    copies[1].wait()
    for b in range(blk_count):
        block = kept[b]
        for c in range(groups):
            here = (coarse[b] - first) == c
            rows, lanes = slice(c * columns, (c + 1) * columns), slice(b * panels, (b + 1) * panels)
            masked[rows, lanes] = jnp.where(here, block, jnp.zeros_like(block))
    for copy in copies[2:]:
        copy.wait()
    right = jnp.concatenate([restrict[b] for b in range(blk_count)], axis=1)
    out[...] = lax.dot_general(masked[...], right, NT, preferred_element_type=F32).astype(out.dtype)


def near_kernel(on, begin, ids, counts, density, *rest):
    halos, (blocks, out, extended) = rest[:-3], rest[-3:]
    blk_count, columns, panels = density.shape
    half = halos[0].shape[0]
    slots = ids.shape[0]
    position = lax.axis_index("panel")
    odd = lax.rem(position, 2)
    base = (1 - odd) * half if on else odd * half
    low = odd if on else 1 - odd
    if on:
        halo = halos[0][...]
    else:
        relayed = jnp.logical_or(position == 1, position == lax.axis_size("panel") - 2)
        halo = jnp.where(relayed, halos[1][...], halos[0][...])
    extended[pl.ds(half, blk_count)] = density[...]
    extended[pl.ds((1 - low) * (half + blk_count), half)] = halo
    empty = blk_count + 2 * half
    extended[empty] = jnp.zeros((columns, panels), extended.dtype)
    live = lax.broadcasted_iota(jnp.int32, ids.shape, 0) < counts[...]
    slabs = jnp.where(live, ids[...] - (position * blk_count - half), empty)
    slabs = jnp.where(base == 0, slabs[:, :half], slabs[:, half:])
    for at in range(out.shape[0]):
        b = base + begin + at
        left = [extended[slabs[j, begin + at]] for j in range(slots)]
        mid = slots // 2
        turned = jnp.concatenate([blocks[b, j].T for j in range(mid)], axis=0)
        plain = jnp.concatenate([blocks[b, j] for j in range(mid, slots)], axis=1)
        out[at] = lax.dot_general(
            jnp.concatenate(left[mid:], axis=1), plain, NT, preferred_element_type=F32
        ) + lax.dot_general(jnp.concatenate(left[:mid], axis=1), turned, NN, preferred_element_type=F32)


def weights_kernel(masks, coarse, coupling, mark, weights, second):
    groups = coupling.shape[0]
    position = lax.axis_index("panel")
    tile = weights.shape[2:]
    columns = coupling[...]
    where_from = lax.broadcasted_iota(jnp.int32, columns.shape, 1)
    for s, mask in enumerate(masks):
        source = lax.bitwise_xor(position, mask) * groups
        for g in range(groups):
            one = jnp.sum(jnp.where(where_from == source + g, columns, 0.0), axis=1, keepdims=True)
            for c in range(groups):
                weights[c, s * groups + g] = jnp.broadcast_to(one[c : c + 1], tile)
    own = coarse[...] - position * groups
    for b in range(second.shape[0]):
        second[b] = jnp.broadcast_to(own[:, b : b + 1], tile)


def mark_kernel(out):
    out[...] = jnp.zeros_like(out)


def coupled(pieces, weights, c, first, columns):
    terms = []
    for piece in pieces:
        for at in range(0, piece.shape[0], columns):
            row = piece[pl.ds(at, columns)].astype(F32)
            weight = weights[c, first + len(terms)]
            terms.append(row * jnp.concatenate([weight] * (columns // weight.shape[0]), axis=0))
    while len(terms) > 1:
        half = len(terms) // 2
        terms = [terms[i] + terms[i + half] for i in range(half)] + terms[2 * half :]
    return terms[0]


def partial_kernel(weights, *rest):
    pieces, out = rest[:-1], rest[-1]
    for c in range(out.shape[0]):
        out[c] = coupled(pieces, weights, c, 0, out.shape[1])


def far_kernel(cuts, weights, second, evaluate, known, early, last, *rest):
    near, out = rest[:-1], rest[-1]
    blk_count, columns, panels = out.shape
    groups, slots = weights.shape[:2]
    local = []
    for c in range(groups):
        total = known[c] + coupled((early, last), weights, c, slots // 2, columns)
        local.append(total.astype(BF16))
    left = jnp.concatenate(local, axis=0)
    half = blk_count // 2
    odd = lax.rem(lax.axis_index("panel"), 2)
    for (on, begin, end), part in zip(cuts, near):
        base = ((1 - odd) * half if on else odd * half) + begin
        for at in range(0, end - begin, 2):
            right = jnp.concatenate([evaluate[base + at], evaluate[base + at + 1]], axis=1)
            both = lax.dot_general(left, right, NN, preferred_element_type=F32)
            for i in (0, 1):
                b = base + at + i
                pick = jnp.concatenate([second[b]] * (columns // second.shape[1]), axis=0)
                lanes = slice(i * panels, (i + 1) * panels)
                far = both[:columns, lanes]
                for c in range(1, groups):
                    far = jnp.where(pick == c, both[c * columns : (c + 1) * columns, lanes], far)
                out[b] = (part[at + i] + far).astype(out.dtype)


def on_chip(*arrays):
    return [pltpu.with_memory_space_constraint(x, pltpu.VMEM) for x in arrays]


def in_hbm(*arrays):
    return [pltpu.with_memory_space_constraint(x, pltpu.HBM) for x in arrays]


def room(mebibytes):
    return pltpu.CompilerParams(vmem_limit_bytes=mebibytes << 20)


def cost(flops, moved):
    return pl.CostEstimate(flops=flops, bytes_accessed=moved, transcendentals=0)


def exchange(x, step):
    count = lax.axis_size("panel")
    return lax.ppermute(x, "panel", [(i, i ^ step) for i in range(count)])


def off_pairs(count):
    goes = {0: 1, 1: 2, 2: 0, count - 3: count - 1, count - 1: count - 2, count - 2: count - 3}
    for i in range(3, count - 4, 2):
        goes[i], goes[i + 1] = i + 1, i
    return sorted(goes.items())


def body(density, near_blocks, neighbours, counts, coarse_map, restrict, evaluate, coupling):
    blk_count, columns, panels = density.shape
    terms = restrict.shape[1]
    groups = coupling.shape[0]
    half = blk_count // 2
    count = lax.axis_size("panel")
    position = lax.axis_index("panel")
    odd = lax.rem(position, 2)

    rounds = rounds_of(count)
    masks = [0]
    for together in rounds:
        masks = masks + [mask ^ step for step in together for mask in masks]

    half_shape = (half, columns, panels)
    chunks = 4
    moments, kept, to_chip, to_off = pl.pallas_call(
        functools.partial(moments_kernel, chunks),
        out_shape=(
            pltpu.VMEM((groups * columns, terms), BF16),
            pltpu.VMEM(density.shape, BF16),
            pltpu.VMEM(half_shape, BF16),
            pltpu.VMEM(half_shape, BF16),
        ),
        in_specs=[HBM] * 3,
        out_specs=(VMEM,) * 4,
        scratch_shapes=[
            pltpu.SMEM(coarse_map.shape, jnp.int32),
            pltpu.VMEM(restrict.shape, BF16),
            pltpu.VMEM((groups * columns, blk_count * panels), BF16),
            pltpu.SemaphoreType.DMA((2 + chunks,)),
        ],
        compiler_params=room(8),
        cost_estimate=cost(10**10, 10**6),
        name="moments",
    )(*in_hbm(coarse_map, density, restrict))

    pieces = [moments]
    for at, together in enumerate(rounds[:-1]):
        sent = pieces[0] if at == 0 else jnp.concatenate(pieces, axis=0)
        for step in together:
            pieces.append(exchange(sent, step))
    lasts = []
    for part in (pieces[:-2], pieces[-2:]):
        sent = jnp.concatenate(part, axis=0)
        lasts.append(exchange(sent, 1))

    chip_halo = exchange(to_chip, 1)
    off_halo = lax.ppermute(to_off, "panel", off_pairs(count))
    relay = exchange(off_halo, 1)

    make_mark = pl.pallas_call(
        mark_kernel,
        out_shape=pltpu.VMEM((8, 128), F32),
        out_specs=VMEM,
        compiler_params=room(1),
        cost_estimate=cost(10**11, 10**6),
        name="mark",
    )
    mark = make_mark()
    make_weights = pl.pallas_call(
        functools.partial(weights_kernel, masks),
        out_shape=(
            pltpu.VMEM((groups, groups * count, 8, 128), F32),
            pltpu.VMEM((blk_count, 8, 128), jnp.int32),
        ),
        in_specs=[VMEM] * 3,
        out_specs=(VMEM, VMEM),
        compiler_params=room(4),
        cost_estimate=cost(10**9, 10**6),
        name="weights",
    )
    weights, second = make_weights(*on_chip(coarse_map.reshape(1, blk_count), coupling, mark))

    ids = neighbours.T
    live_counts = counts.reshape(1, blk_count)
    near = []
    cuts = [(on, begin * half // 8, end * half // 8) for on, begin, end in CUTS]
    for on, begin, end in cuts:
        halos = (chip_halo,) if on else (off_halo, relay)
        call = pl.pallas_call(
            functools.partial(near_kernel, on, begin),
            out_shape=pltpu.VMEM((end - begin, columns, panels), F32),
            in_specs=[VMEM] * (4 + len(halos)),
            out_specs=VMEM,
            scratch_shapes=[
                pltpu.VMEM((blk_count + 2 * half + 1, columns, panels), BF16),
            ],
            compiler_params=room(4),
            cost_estimate=cost(2 * 10**9, 10**6),
        )
        near.append(call(*on_chip(ids, live_counts, kept, *halos, near_blocks)))

    make_partial = pl.pallas_call(
        partial_kernel,
        out_shape=pltpu.VMEM((groups, columns, panels), F32),
        in_specs=[VMEM] * (1 + len(pieces)),
        out_specs=VMEM,
        compiler_params=room(4),
        cost_estimate=cost(10**9, 10**6),
        name="partial",
    )
    known = make_partial(*on_chip(weights, *pieces))

    return pl.pallas_call(
        functools.partial(far_kernel, cuts),
        out_shape=jax.ShapeDtypeStruct(density.shape, BF16),
        in_specs=[VMEM] * (6 + len(near)),
        out_specs=VMEM,
        compiler_params=room(4),
        cost_estimate=cost(10**9, 10**6),
        name="far",
    )(*on_chip(weights, second, evaluate, known, *lasts, *near))


CUTS = ((True, 0, 8), (False, 0, 4), (False, 4, 8))


def rounds_of(count):
    return [[(1 << bit) | 1] for bit in range(count.bit_length() - 2, 2, -1)] + [[7, 5, 3], [1]]


def solution(mesh):
    placed = (
        P(("grp", "panel"), None, None),
        P(("grp", "panel"), None, None, None),
        P(("grp", "panel"), None),
        P(("grp", "panel")),
        P(("grp", "panel")),
        P(("grp", "panel"), None, None),
        P(("grp", "panel"), None, None),
        P(("grp", "panel"), None),
    )
    return jax.shard_map(
        body,
        mesh=mesh,
        in_specs=placed,
        out_specs=P(("grp", "panel"), None, None),
        check_vma=False,
    )
```
